32 devices in a mesh: rows: 4 (over x, core), cols: 8 (over z, y).
Axes of the slice: x: 2, y: 2, z: 4, core: 2. Of those that a mesh axis runs over, the one named last changes fastest.
Arguments:
- design: bfloat16 [4096, 8192], P('rows', 'cols'), may hold values from -6 to 6
- theta: float32 [8192], P('cols'), may hold values from -0.0625 to 0.0625
- feature_scale: float32 [8192], P('cols'), may hold values from 0.05 to 2
- labels: int32 [4096], P('rows'), may hold values 0 or 1
- psi: bfloat16 [1024, 256], replicated, may hold values from -0.1875 to 0.1875
- phi: float32 [512, 256], replicated, may hold values from -0.25 to 0.25
Outputs:
- newton_step: float32 [8192], P('cols')
- sketch: float32 [256, 8192], P(None, 'cols')
The draws below stay inside these ranges and needn't reach their ends.
All inputs are finite; a program needn't handle non-finite values. No bound on the sum of `labels` on one device may be relied on, other than what follows from the above.
Results may differ from the reference program's by a relative error of at most 0.0085.
Values sent between devices are 32-bit elements; how exact they have to be, the bound alone decides.
A program may use at most 128 MiB of HBM per device.

```python
import math
import jax
import jax.numpy as jnp
from jax import lax

F = 8192
S = 256
R_DEV = 1024
ITERS = 10
SAMPLES = 4096
LEVELS = 2
N_ROWS = 4


def with_ends(drawn, rng, least, high):
    longest = drawn.shape.index(max(drawn.shape))
    spots = []
    for shift in (0, 1):
        where = [jax.random.randint(jax.random.fold_in(rng, axis), (), 0, length) for axis, length in enumerate(drawn.shape)]
        where[longest] = (where[longest] + shift) % drawn.shape[longest]
        spots.append(tuple(where))
    return drawn.at[spots[0]].set(least).at[spots[1]].set(high)


def steps_of(rng, shape, shards, smallest, top_value):
    level, own = 1.0, jax.random.fold_in(rng, 6)
    for axis_at, parts in shards:
        draws = jnp.exp(jax.random.uniform(jax.random.fold_in(own, axis_at), (parts,), jnp.float32, smallest / len(shards), top_value / len(shards)))
        level = level * jnp.repeat(draws, shape[axis_at] // parts).reshape([-1 if axis == axis_at else 1 for axis in range(len(shape))])
    return level


def noise(own_key, extent, deviation, most, split=(), held_as=jnp.bfloat16):
    factor_of = steps_of(own_key, extent, split, -0.22, 0.18) if split else 1.0
    result = jax.random.normal(own_key, extent, jnp.float32) * deviation * factor_of
    return jnp.minimum(jnp.maximum(result, -most), most).astype(held_as)


def setup_inputs(seed: int = 0) -> dict:
    key_list = jax.random.split(jax.random.key(seed), 7)
    design = noise(key_list[0], (SAMPLES, F), 1.0, 6.0, ((0, 4), (1, 8)))
    theta = noise(key_list[1], (F,), F ** -0.5, 0.0625, ((0, 8),), jnp.float32)
    feature_scale = jnp.clip(jnp.exp(math.log(2.0) - 3.6888794 * jax.random.uniform(key_list[2], (F,), jnp.float32) ** steps_of(key_list[2], (F,), ((0, 8),), -0.2, 0.2)), 0.05, 2.0)
    labels = with_ends((jax.random.randint(key_list[3], (SAMPLES,), 0, 2) < 1).astype(jnp.int32), jax.random.fold_in(key_list[3], 1), 0, 1)
    psi = noise(key_list[4], (R_DEV, S), R_DEV ** -0.5, 0.1875)
    phi = noise(key_list[5], (2 * S, S), (2 * S) ** -0.5, 0.25, (), jnp.float32)
    return dict(design=design, theta=theta, feature_scale=feature_scale, labels=labels, psi=psi, phi=phi)


damping = 0.01
shrink_share = 0.05
highest = lax.Precision.HIGHEST

def shrink_weights(range_rows):
    width = range_rows.shape[1]
    moment = jnp.dot(range_rows.T, range_rows, precision=highest)
    ridge = shrink_share * jnp.trace(moment) / width
    factor = jnp.linalg.cholesky(moment + ridge * jnp.eye(width, dtype=jnp.float32))
    return jax.scipy.linalg.solve_triangular(factor, range_rows.T, lower=True)

def reference(design, theta, feature_scale, labels, psi, phi):
    samples = design.shape[0]
    features = design.shape[1]
    scaled_theta = (theta * feature_scale).astype(jnp.bfloat16)
    margins = jnp.dot(design.astype(jnp.float32), scaled_theta.astype(jnp.float32), preferred_element_type=jnp.float32)
    chance = jax.nn.sigmoid(margins)
    weight = chance * (1.0 - chance)
    misfit = (chance - labels.astype(jnp.float32)).astype(jnp.bfloat16)
    gradient = feature_scale * jnp.dot(misfit.astype(jnp.float32), design.astype(jnp.float32), preferred_element_type=jnp.float32) / samples + damping * theta

    def local_sketch(pieces):
        block, block_weight = pieces
        rows_scaled = (block.astype(jnp.float32) * jnp.sqrt(block_weight)[:, None] * feature_scale[None, :]).astype(jnp.bfloat16)
        mixed_cols = jnp.dot(rows_scaled.T.astype(jnp.float32), psi.astype(jnp.float32), preferred_element_type=jnp.float32).astype(jnp.bfloat16)
        range_rows = jnp.dot(rows_scaled.astype(jnp.float32), mixed_cols.astype(jnp.float32), preferred_element_type=jnp.float32)
        leaf_weights = shrink_weights(range_rows).astype(jnp.bfloat16)
        return jnp.dot(leaf_weights.astype(jnp.float32), rows_scaled.astype(jnp.float32), preferred_element_type=jnp.float32)

    def merge_pair(stacked):
        gram = jnp.dot(stacked, stacked.T, precision=highest)
        range_rows = jnp.dot(gram, phi, precision=highest)
        return jnp.dot(shrink_weights(range_rows), stacked, precision=highest)
    sketches = lax.map(local_sketch, (design.reshape(N_ROWS, R_DEV, features), weight.reshape(N_ROWS, R_DEV)))
    for level_index in range(LEVELS):
        pairs_now = sketches.shape[0] // 2
        sketches = lax.map(merge_pair, sketches.reshape(pairs_now, 2 * S, features))
    sketch = sketches[0]
    kernel = jnp.dot(sketch, sketch.T, precision=highest) + damping * samples * jnp.eye(S, dtype=jnp.float32)
    kernel_factor = jnp.linalg.cholesky(kernel)

    def precondition(vector):
        projected = jnp.dot(sketch, vector, precision=highest)
        solved = jax.scipy.linalg.cho_solve((kernel_factor, True), projected)
        return (vector - jnp.dot(solved, sketch, precision=highest)) / damping

    def hessian(vector):
        rounded = (feature_scale * vector).astype(jnp.bfloat16)
        forward_rows = jnp.dot(design.astype(jnp.float32), rounded.astype(jnp.float32), preferred_element_type=jnp.float32)
        inner = (weight * forward_rows).astype(jnp.bfloat16)
        return feature_scale * jnp.dot(inner.astype(jnp.float32), design.astype(jnp.float32), preferred_element_type=jnp.float32) / samples + damping * vector
    solution = jnp.zeros_like(gradient)
    residual = gradient
    search = precondition(residual)
    agreement = jnp.sum(residual * search)
    for turn_index in range(ITERS):
        product = hessian(search)
        step_size = agreement / jnp.sum(search * product)
        solution = solution + step_size * search
        residual = residual - step_size * product
        smoothed = precondition(residual)
        agreement_next = jnp.sum(residual * smoothed)
        search = smoothed + agreement_next / agreement * search
        agreement = agreement_next
    return (solution, sketch)
```

```python
import functools

import jax
import jax.numpy as jnp
from jax import lax
from jax.experimental import pallas as pl
from jax.experimental.pallas import tpu as pltpu
from jax.sharding import PartitionSpec as P

ITERS = 10
BLOCK = 32
LANES = 128

damping = 0.01
shrink_share = 0.05
highest = lax.Precision.HIGHEST
MESH = pl.DeviceIdType.MESH
VMEM_SPEC = pl.BlockSpec(memory_space=pltpu.VMEM)
f32 = jnp.float32
bf16 = jnp.bfloat16


def iota(shape, axis):
    return lax.broadcasted_iota(jnp.int32, shape, axis)


def split3(value):
    high = value.astype(bf16)
    rest = value - high.astype(f32)
    mid = rest.astype(bf16)
    low = (rest - mid.astype(f32)).astype(bf16)
    return high, mid, low


def nn(a, b, precision=None):
    return lax.dot_general(a, b, (((1,), (0,)), ((), ())), precision=precision, preferred_element_type=f32)


def nt(a, b, precision=None):
    return lax.dot_general(a, b, (((1,), (1,)), ((), ())), precision=precision, preferred_element_type=f32)


def tn(a, b, precision=None):
    return lax.dot_general(a, b, (((0,), (0,)), ((), ())), precision=precision, preferred_element_type=f32)


def inverse_factor(work, out, width):
    def block_step(b, carry):
        start = pl.multiple_of(b * BLOCK, BLOCK)
        rows = work[pl.ds(start, BLOCK), :]
        left = rows[:, :width]
        shifted = pltpu.roll(left, width - start, 1)[:, :LANES]
        lane = iota((BLOCK, LANES), 1)
        sub = iota((BLOCK, LANES), 0)
        small = jnp.where(lane < BLOCK, shifted, jnp.where(lane == sub + BLOCK, 1.0, 0.0))
        diag = jnp.ones((BLOCK, 1), f32)
        mixing = jnp.zeros((BLOCK, 1), f32)
        sub1 = iota((BLOCK, 1), 0)
        for j in range(0, BLOCK, 2):
            col0, col1 = small[:, j : j + 1], small[:, j + 1 : j + 2]
            row0, row1 = small[j : j + 1, :], small[j + 1 : j + 2, :]
            p00 = small[j : j + 1, j : j + 1]
            p01 = small[j : j + 1, j + 1 : j + 2]
            p11 = small[j + 1 : j + 2, j + 1 : j + 2]
            det = p00 * p11 - p01 * p01
            diag = jnp.where(sub1 == j, p00, jnp.where(sub1 == j + 1, det / p00, diag))
            mixing = jnp.where(sub1 == j + 1, p01 / p00, mixing)
            if j + 2 < BLOCK:
                share = 1.0 / det
                new0 = (p11 * row0 - p01 * row1) * share
                new1 = (p00 * row1 - p01 * row0) * share
                below0 = jnp.where(sub1 > j + 1, col0, 0.0)
                below1 = jnp.where(sub1 > j + 1, col1, 0.0)
                small = small - below0 * new0 - below1 * new1
        small = (small - mixing * pltpu.roll(small, 1, 0)) * lax.rsqrt(diag)
        inverse = small[:, BLOCK : 2 * BLOCK]
        panel = nn(inverse, rows, highest)
        out[pl.ds(start, BLOCK), :] = panel[:, width:]
        lanes = iota((BLOCK, width), 1)
        below = jnp.where(lanes >= start + BLOCK, panel[:, :width], 0.0)
        ph, pm, pw = split3(below)
        qh, qm, qw = split3(panel)
        left_side = jnp.concatenate([ph, ph, pm, ph, pw, pm], 0)
        right_side = jnp.concatenate([qh, qm, qh, qw, qh, qm], 0)
        work[...] -= tn(left_side, right_side)
        return carry

    lax.fori_loop(0, width // BLOCK, block_step, 0)


def load_matrix(work, matrix, ridge):
    width = matrix.shape[0]
    eye = jnp.where(iota((width, width), 0) == iota((width, width), 1), 1.0, 0.0)
    if ridge is None:
        ridge = shrink_share * jnp.sum(matrix * eye) / width
    work[:, :width] = matrix + ridge * eye
    work[:, width:] = eye


def leaf_kernel(y_ref, w_ref, work, inv):
    y = y_ref[...]
    width = y.shape[1]
    load_matrix(work, tn(y, y, highest), None)
    inverse_factor(work, inv, width)
    w_ref[...] = nt(inv[...], y, highest).astype(bf16)


def leaf_weights_of(y):
    rows, width = y.shape
    return pl.pallas_call(
        leaf_kernel,
        out_shape=jax.ShapeDtypeStruct((width, rows), bf16),
        in_specs=[VMEM_SPEC],
        out_specs=VMEM_SPEC,
        scratch_shapes=[pltpu.VMEM((width, 2 * width), f32), pltpu.VMEM((width, width), f32)],
    )(y)


def merge_kernel(inner_ridge, g_ref, phi_ref, w_ref, k_ref, work, inv):
    width = phi_ref.shape[1]
    aa, ab, bb = (g_ref[i * width : (i + 1) * width, :] for i in range(3))
    top, low = phi_ref[:width, :], phi_ref[width:, :]
    y_top = nn(aa, top, highest) + nn(ab, low, highest)
    y_low = tn(ab, top, highest) + nn(bb, low, highest)
    load_matrix(work, tn(y_top, y_top, highest) + tn(y_low, y_low, highest), None)
    inverse_factor(work, inv, width)
    w_top = nt(inv[...], y_top, highest)
    w_low = nt(inv[...], y_low, highest)
    w_ref[:, :width] = w_top
    w_ref[:, width:] = w_low
    wg_top = nn(w_top, aa, highest) + nt(w_low, ab, highest)
    wg_low = nn(w_top, ab, highest) + nn(w_low, bb, highest)
    own_gram = nt(wg_top, w_top, highest) + nt(wg_low, w_low, highest)
    if inner_ridge is None:
        k_ref[...] = own_gram
        return
    load_matrix(work, own_gram, inner_ridge)
    inverse_factor(work, inv, width)
    k_ref[...] = tn(inv[...], inv[...], highest)


def merge_weights_of(gram, phi, inner_ridge):
    width = phi.shape[1]
    return pl.pallas_call(
        functools.partial(merge_kernel, inner_ridge),
        out_shape=(
            jax.ShapeDtypeStruct((width, 2 * width), f32),
            jax.ShapeDtypeStruct((width, width), f32),
        ),
        in_specs=[VMEM_SPEC] * 2,
        out_specs=(VMEM_SPEC,) * 2,
        scratch_shapes=[pltpu.VMEM((width, 2 * width), f32), pltpu.VMEM((width, width), f32)],
    )(gram, phi)


def small_sum_kernel(axis, n, x_ref, o_ref, land, send_sem, recv_sem):
    me = lax.axis_index(axis)
    barrier = pltpu.get_barrier_semaphore()
    for d in range(1, n):
        pl.semaphore_signal(barrier, inc=1, device_id={axis: lax.rem(me + d, n)}, device_id_type=MESH)
    pl.semaphore_wait(barrier, n - 1)
    for d in range(1, n):
        pltpu.make_async_remote_copy(
            x_ref, land.at[me], send_sem.at[d], recv_sem.at[me],
            device_id={axis: lax.rem(me + d, n)}, device_id_type=MESH,
        ).start()
    land[me] = x_ref[...]
    for d in range(1, n):
        source = lax.rem(me + n - d, n)
        pltpu.make_async_remote_copy(
            x_ref, land.at[source], send_sem.at[d], recv_sem.at[source],
            device_id={axis: lax.rem(me + d, n)}, device_id_type=MESH,
        ).wait()
    total = land[0]
    for i in range(1, n):
        total = total + land[i]
    o_ref[...] = total


def small_sum(x, axis, collective_id):
    n = lax.axis_size(axis)
    return pl.pallas_call(
        functools.partial(small_sum_kernel, axis, n),
        out_shape=jax.ShapeDtypeStruct(x.shape, f32),
        in_specs=[VMEM_SPEC],
        out_specs=VMEM_SPEC,
        scratch_shapes=[
            pltpu.VMEM((n, *x.shape), f32),
            pltpu.SemaphoreType.DMA((n,)),
            pltpu.SemaphoreType.DMA((n,)),
        ],
        compiler_params=pltpu.CompilerParams(collective_id=collective_id, has_side_effects=True),
    )(x)


def big_sum_kernel(n, share, x_ref, o_ref, land1, out1, land2, full, s1, r1, s2, r2, sa, ra, sb, rb, sc, rc, sd, rd):
    me = lax.axis_index("cols")
    position = lax.axis_index("rows")
    base = position // share * share
    own = lax.rem(position, share)
    side, line, far = lax.rem(me, 2), me // 2, n // 2
    other = 1 - side
    halves = max(share // 2, 1)
    chunk = x_ref.shape[0] // (n * share)

    def rows_of(line_at, side_at, sub):
        return pl.ds(pl.multiple_of((sub * n + line_at * 2 + side_at) * chunk, chunk), chunk)

    def along(t):
        return lax.rem(line + t, far)

    def back(t):
        return lax.rem(line + far - t, far)

    def sub_of(e, mine):
        return lax.rem(mine + share - 2 * e, share)

    pair = {"rows": position, "cols": line * 2 + other}
    sibling = {"rows": base + own + 1 - 2 * lax.rem(own, 2), "cols": me}
    sibling_own = own + 1 - 2 * lax.rem(own, 2)

    def peer(t, e):
        return {"rows": base + lax.rem(own + 2 * e, share), "cols": along(t) * 2 + side}

    spread = [(t, e) for e in range(halves) for t in range(far)]
    greeted = [pair] + [peer(t, e) for t, e in spread if t or e] + ([sibling] if share > 1 else [])
    barrier = pltpu.get_barrier_semaphore()
    for device in greeted:
        pl.semaphore_signal(barrier, inc=1, device_id=device, device_id_type=MESH)
    pl.semaphore_wait(barrier, len(greeted))

    def copy(src, dst, send, recv, device):
        return pltpu.make_async_remote_copy(src, dst, send, recv, device_id=device, device_id_type=MESH)

    first = []
    for t in range(far):
        rows = rows_of(along(t + 1), other, own)
        first.append(copy(x_ref.at[rows], land1.at[t], s1.at[t], r1.at[t], pair))
        first[-1].start()
    second = []
    for t in range(far):
        first[t].wait_recv()
        total = land1[t] + x_ref[rows_of(along(t + 1), side, own), :]
        if t + 1 < far:
            out1[t] = total
            second.append(copy(out1.at[t], land2.at[t], s2.at[t], r2.at[t], peer(t + 1, 0)))
            second[-1].start()
    for t in range(far - 1):
        second[t].wait_recv()
        total = total + land2[t]
    mine = rows_of(line, side, own)
    full[mine, :] = total

    outward, started = {}, []
    for t, e in spread:
        if t or e:
            outward[t, e] = copy(full.at[mine], full.at[mine], sa.at[t, e], ra.at[t, e], peer(t, e))
            outward[t, e].start()
    for t, e in spread:
        rows = rows_of(back(t), side, sub_of(e, own))
        if t or e:
            copy(full.at[mine], full.at[rows], sa.at[t, e], ra.at[t, e], peer(t, e)).wait_recv()
        started.append(copy(full.at[rows], full.at[rows], sb.at[t, e], rb.at[t, e], pair))
        started[-1].start()
        if share > 1:
            started.append(copy(full.at[rows], full.at[rows], sc.at[t, e], rc.at[t, e], sibling))
            started[-1].start()
    for t, e in spread:
        rows = rows_of(back(t), other, sub_of(e, own))
        copy(full.at[rows], full.at[rows], sb.at[t, e], rb.at[t, e], pair).wait_recv()
        if share > 1:
            started.append(copy(full.at[rows], full.at[rows], sd.at[t, e], rd.at[t, e], sibling))
            started[-1].start()
    if share > 1:
        for t, e in spread:
            rows = rows_of(back(t), side, sub_of(e, sibling_own))
            copy(full.at[rows], full.at[rows], sc.at[t, e], rc.at[t, e], sibling).wait_recv()
            rows = rows_of(back(t), other, sub_of(e, sibling_own))
            copy(full.at[rows], full.at[rows], sd.at[t, e], rd.at[t, e], sibling).wait_recv()
    for sent in first + second + list(outward.values()) + started:
        sent.wait_send()
    o_ref[...] = full[...]


def big_sum(x, share, collective_id):
    n = lax.axis_size("cols")
    while share > 1 and x.shape[0] % (n * share * 8):
        share //= 2
    chunk = x.shape[0] // (n * share)
    far, halves = n // 2, max(share // 2, 1)
    dma = pltpu.SemaphoreType.DMA
    return pl.pallas_call(
        functools.partial(big_sum_kernel, n, share),
        out_shape=jax.ShapeDtypeStruct(x.shape, f32),
        in_specs=[VMEM_SPEC],
        out_specs=VMEM_SPEC,
        scratch_shapes=[
            pltpu.VMEM((far, chunk, x.shape[1]), f32),
            pltpu.VMEM((far, chunk, x.shape[1]), f32),
            pltpu.VMEM((far, chunk, x.shape[1]), f32),
            pltpu.VMEM(x.shape, f32),
        ]
        + [dma((far,))] * 4
        + [dma((far, halves))] * 8,
        compiler_params=pltpu.CompilerParams(collective_id=collective_id, has_side_effects=True),
    )(x)


PIECES = 8


def swap_kernel(stride, x_ref, o_ref, land, ss, rs, fs, fr):
    position = lax.axis_index("rows")
    core = lax.rem(position, 2)
    partner = {"rows": position + stride - 2 * stride * lax.rem(position // stride, 2)}
    sibling = {"rows": position + 1 - 2 * core}
    piece = x_ref.shape[0] // (2 * PIECES)
    barrier = pltpu.get_barrier_semaphore()
    for device in (partner, sibling):
        pl.semaphore_signal(barrier, inc=1, device_id=device, device_id_type=MESH)
    pl.semaphore_wait(barrier, 2)

    def rows_of(half, i):
        return pl.ds(pl.multiple_of((half * PIECES + i) * piece, piece), piece)

    sent = []
    for i in range(PIECES):
        rows = rows_of(core, i)
        sent.append(
            pltpu.make_async_remote_copy(
                x_ref.at[rows], land.at[rows], ss.at[i], rs.at[i], device_id=partner, device_id_type=MESH
            )
        )
        sent[-1].start()
    passed = []
    for i in range(PIECES):
        rows = rows_of(core, i)
        sent[i].wait_recv()
        passed.append(
            pltpu.make_async_remote_copy(
                land.at[rows], land.at[rows], fs.at[i], fr.at[i], device_id=sibling, device_id_type=MESH
            )
        )
        passed[-1].start()
    for i in range(PIECES):
        rows = rows_of(1 - core, i)
        pltpu.make_async_remote_copy(
            land.at[rows], land.at[rows], fs.at[i], fr.at[i], device_id=sibling, device_id_type=MESH
        ).wait_recv()
    for copy in sent + passed:
        copy.wait_send()
    o_ref[...] = land[...]


def split_swap(x, stride, collective_id):
    dma = pltpu.SemaphoreType.DMA
    return pl.pallas_call(
        functools.partial(swap_kernel, stride),
        out_shape=jax.ShapeDtypeStruct(x.shape, f32),
        in_specs=[VMEM_SPEC],
        out_specs=VMEM_SPEC,
        scratch_shapes=[pltpu.VMEM(x.shape, f32)] + [dma((PIECES,))] * 4,
        compiler_params=pltpu.CompilerParams(collective_id=collective_id, has_side_effects=True),
    )(x)


def fold(value):
    total = value[:, :LANES]
    for i in range(1, value.shape[1] // LANES):
        total = total + value[:, i * LANES : (i + 1) * LANES]
    return total


def total_of(value):
    return jnp.sum(value, axis=1, keepdims=True)


def three_rows(value):
    wide = jnp.broadcast_to(value, (16, value.shape[1]))
    high = wide.astype(bf16).astype(f32)
    mid = (wide - high).astype(bf16).astype(f32)
    low = wide - high - mid
    sub = iota(wide.shape, 0)
    return jnp.where(sub == 0, high, jnp.where(sub == 1, mid, jnp.where(sub == 2, low, 0.0))).astype(bf16)


def many_rows(value):
    return jnp.broadcast_to(value, (16, value.shape[1])).astype(bf16)


def solve_kernel(
    n_rows, n_cols, samples,
    design, weight, scale, theta, misfit, sketch, kinv, out,
    s3, k3, a_send, a_land, b_send, b_land, c_send, c_land,
    a_ss, a_rs, b_ss, b_rs, c_ss, c_rs,
):
    width = sketch.shape[0]
    here = {"rows": lax.axis_index("rows"), "cols": lax.axis_index("cols")}
    sizes = {"rows": n_rows, "cols": n_cols}

    def peer(axis, d):
        return lax.rem(here[axis] + d, sizes[axis])

    barrier = pltpu.get_barrier_semaphore()
    for axis, n in sizes.items():
        for d in range(1, n):
            pl.semaphore_signal(barrier, inc=1, device_id={axis: peer(axis, d)}, device_id_type=MESH)
    pl.semaphore_wait(barrier, n_rows + n_cols - 2)

    def exchange(axis, value, parity, send, land, ss, rs):
        n, me = sizes[axis], here[axis]
        send[...] = value
        for d in range(1, n):
            pltpu.make_async_remote_copy(
                send, land.at[parity, me], ss.at[d], rs.at[parity, me],
                device_id={axis: peer(axis, d)}, device_id_type=MESH,
            ).start()
        land[parity, me] = value
        for d in range(1, n):
            source = peer(axis, n - d)
            pltpu.make_async_remote_copy(
                send, land.at[parity, source], ss.at[d], rs.at[parity, source],
                device_id={axis: peer(axis, d)}, device_id_type=MESH,
            ).wait()
        total = land[parity, 0]
        for i in range(1, n):
            total = total + land[parity, i]
        return total

    def precondition(vector, parity):
        left = three_rows(vector)
        parts = nt(left, s3[0]) + nt(left, s3[1]) + nt(left, s3[2])
        projected = jnp.sum(parts, axis=0, keepdims=True)
        both = jnp.concatenate([projected, fold(vector * vector)], 1)
        both = exchange("cols", both, parity, c_send, c_land, c_ss, c_rs)
        projected = both[:, :width]
        left = three_rows(projected)
        solved = jnp.sum(nn(left, k3[0]) + nn(left, k3[1]) + nn(left, k3[2]), axis=0, keepdims=True)
        left = three_rows(solved)
        removed = jnp.sum(nn(left, s3[0]) + nn(left, s3[1]) + nn(left, s3[2]), axis=0, keepdims=True)
        agreement = (total_of(both[:, width:]) - total_of(projected * solved)) / damping
        return (vector - removed) / damping, agreement

    def backward(inner, extra, parity):
        part = nn(many_rows(inner), design[...])[:1]
        both = jnp.concatenate([part, extra], 1)
        both = exchange("rows", both, parity, b_send, b_land, b_ss, b_rs)
        return scale[...] * both[:, : part.shape[1]] / samples, total_of(both[:, part.shape[1] :])

    for i, piece in enumerate(split3(sketch[...])):
        s3[i] = piece
    for i, piece in enumerate(split3(kinv[...])):
        k3[i] = piece

    scaled, _ = backward(misfit[...], jnp.zeros((1, LANES), f32), 1)
    residual = scaled + damping * theta[...]
    search, agreement = precondition(residual, 1)

    def advance(turn, search, residual, answer, agreement):
        parity = lax.rem(turn, 2)
        part = nt(many_rows(scale[...] * search), design[...])[:1]
        both = jnp.concatenate([part, fold(search * search)], 1)
        both = exchange("cols", both, parity, a_send, a_land, a_ss, a_rs)
        forward = both[:, : part.shape[1]]
        length = total_of(both[:, part.shape[1] :])
        inner = (weight[...] * forward).astype(bf16).astype(f32)
        product, bending = backward(inner, fold(forward * inner), parity)
        product = product + damping * search
        step_size = agreement / (bending / samples + damping * length)
        return residual - step_size * product, answer + step_size * search

    def body(turn, state):
        search, residual, answer, agreement = state
        residual, answer = advance(turn, search, residual, answer, agreement)
        smoothed, following = precondition(residual, lax.rem(turn, 2))
        return smoothed + following / agreement * search, residual, answer, following

    state = (search, residual, jnp.zeros_like(residual), agreement)
    search, residual, answer, agreement = lax.fori_loop(0, ITERS - 1, body, state)
    _, answer = advance(ITERS - 1, search, residual, answer, agreement)
    out[...] = answer


def solve(design, weight, scale, theta, misfit, sketch, kinv, collective_id):
    rows, cols = design.shape
    width = sketch.shape[0]
    n_rows, n_cols = lax.axis_size("rows"), lax.axis_size("cols")
    dma = pltpu.SemaphoreType.DMA
    return pl.pallas_call(
        functools.partial(solve_kernel, n_rows, n_cols, rows * n_rows),
        out_shape=jax.ShapeDtypeStruct((1, cols), f32),
        in_specs=[VMEM_SPEC] * 7,
        out_specs=VMEM_SPEC,
        scratch_shapes=[
            pltpu.VMEM((3, width, cols), bf16),
            pltpu.VMEM((3, width, width), bf16),
            pltpu.VMEM((1, rows + LANES), f32),
            pltpu.VMEM((2, n_cols, 1, rows + LANES), f32),
            pltpu.VMEM((1, cols + LANES), f32),
            pltpu.VMEM((2, n_rows, 1, cols + LANES), f32),
            pltpu.VMEM((1, width + LANES), f32),
            pltpu.VMEM((2, n_cols, 1, width + LANES), f32),
            dma((n_cols,)), dma((2, n_cols)),
            dma((n_rows,)), dma((2, n_rows)),
            dma((n_cols,)), dma((2, n_cols)),
        ],
        compiler_params=pltpu.CompilerParams(collective_id=collective_id, has_side_effects=True),
    )(design, weight, scale, theta, misfit, sketch, kinv)


def swapped(value, axis, stride):
    mask = 2**stride
    pairs = [(source, source ^ mask) for source in range(lax.axis_size(axis))]
    return lax.ppermute(value, axis, pairs)


def on_device(design, theta, feature_scale, labels, psi, phi):
    row_devices = lax.axis_size("rows")
    samples = design.shape[0] * row_devices
    width = psi.shape[1]
    scaled_theta = (theta * feature_scale).astype(bf16)
    part = jnp.dot(design, scaled_theta, preferred_element_type=f32)
    margins = small_sum(part.reshape(-1, LANES), "cols", 0).reshape(-1)
    chance = jax.nn.sigmoid(margins)
    weight = chance * (1.0 - chance)
    misfit = (chance - labels.astype(f32)).astype(bf16).astype(f32)
    rows_scaled = (
        design.astype(f32) * jnp.sqrt(weight)[:, None] * feature_scale[None, :]
    ).astype(bf16)
    mixed_cols = jnp.einsum("rf,rs->fs", rows_scaled, psi, preferred_element_type=f32).astype(bf16)
    range_rows = big_sum(jnp.dot(rows_scaled, mixed_cols, preferred_element_type=f32), 1, 1)
    sketch = jnp.dot(leaf_weights_of(range_rows), rows_scaled, preferred_element_type=f32)
    position = lax.axis_index("rows")
    levels = row_devices.bit_length() - 1
    features = sketch.shape[1]
    for level_bit in range(levels):
        if level_bit:
            sketch = jnp.concatenate([sketch, own_gram], 1)
            partner = split_swap(sketch, 1 << level_bit, 8 + level_bit)
        else:
            partner = swapped(sketch, "rows", level_bit)
        first_low = position // (1 << level_bit) % 2 == 0
        lower_half = jnp.where(first_low, sketch, partner)
        upper_half = jnp.where(first_low, partner, sketch)
        lower, upper = lower_half[:, :features], upper_half[:, :features]
        gram = jnp.dot(lower, upper.T, precision=highest)
        if level_bit:
            gram = big_sum(gram, 2 << level_bit, 2 + level_bit)
            gram = jnp.concatenate([lower_half[:, features:], gram, upper_half[:, features:]], 0)
        else:
            gram = jnp.concatenate(
                [
                    jnp.dot(lower, lower.T, precision=highest),
                    gram,
                    jnp.dot(upper, upper.T, precision=highest),
                ],
                0,
            )
            gram = big_sum(gram, 2, 2)
        last = level_bit + 1 == levels
        weights, own_gram = merge_weights_of(gram, phi, damping * samples if last else None)
        sketch = jnp.dot(weights, jnp.concatenate([lower, upper], 0), precision=highest)
    answer = solve(
        design, weight[None], feature_scale[None], theta[None], misfit[None], sketch, own_gram, 2 + levels
    )
    return answer[0], sketch


def solution(mesh):
    in_specs = (P("rows", "cols"), P("cols"), P("cols"), P("rows"), P(), P())
    out_specs = (P("cols"), P(None, "cols"))
    return jax.shard_map(
        on_device, mesh=mesh, in_specs=in_specs, out_specs=out_specs, check_vma=False
    )
```

```python
import functools

import jax
import jax.numpy as jnp
from jax import lax
from jax.experimental import pallas as pl
from jax.experimental.pallas import tpu as pltpu
from jax.sharding import PartitionSpec as P

ITERS = 10
BLOCK = 64
LANES = 128

damping = 0.01
shrink_share = 0.05
highest = lax.Precision.HIGHEST
MESH = pl.DeviceIdType.MESH
VMEM_SPEC = pl.BlockSpec(memory_space=pltpu.VMEM)
f32 = jnp.float32
bf16 = jnp.bfloat16


def iota(shape, axis):
    return lax.broadcasted_iota(jnp.int32, shape, axis)


def split3(value):
    high = value.astype(bf16)
    rest = value - high.astype(f32)
    mid = rest.astype(bf16)
    low = (rest - mid.astype(f32)).astype(bf16)
    return high, mid, low


def nn(a, b, precision=None):
    return lax.dot_general(a, b, (((1,), (0,)), ((), ())), precision=precision, preferred_element_type=f32)


def nt(a, b, precision=None):
    return lax.dot_general(a, b, (((1,), (1,)), ((), ())), precision=precision, preferred_element_type=f32)


def tn(a, b, precision=None):
    return lax.dot_general(a, b, (((0,), (0,)), ((), ())), precision=precision, preferred_element_type=f32)


def inverse_factor(work, out, width):
    def block_step(b, carry):
        start = pl.multiple_of(b * BLOCK, BLOCK)
        rows = work[pl.ds(start, BLOCK), :]
        left = rows[:, :width]
        shifted = pltpu.roll(left, width - start, 1)[:, :LANES]
        lane = iota((BLOCK, LANES), 1)
        sub = iota((BLOCK, LANES), 0)
        small = jnp.where(lane < BLOCK, shifted, jnp.where(lane == sub + BLOCK, 1.0, 0.0))
        tiles = [small[i : i + 8] for i in range(0, BLOCK, 8)]
        sub8 = iota((8, LANES), 0)
        diags, mixings = [], []
        for j in range(0, BLOCK, 2):
            at, r = j // 8, j % 8
            if r == 0:
                diag = jnp.ones((8, LANES), f32)
                mixing = jnp.zeros((8, LANES), f32)
            wide0 = [jnp.broadcast_to(tile[:, j : j + 1], (8, LANES)) for tile in tiles[at:]]
            wide1 = [jnp.broadcast_to(tile[:, j + 1 : j + 2], (8, LANES)) for tile in tiles[at:]]
            row0, row1 = (jnp.broadcast_to(tiles[at][r + i : r + i + 1], (8, LANES)) for i in range(2))
            p00 = jnp.broadcast_to(wide0[0][r : r + 1], (8, LANES))
            p01 = jnp.broadcast_to(wide0[0][r + 1 : r + 2], (8, LANES))
            p11 = jnp.broadcast_to(wide1[0][r + 1 : r + 2], (8, LANES))
            det = p00 * p11 - p01 * p01
            ratio = 1.0 / p00
            diag = jnp.where(sub8 == r, p00, jnp.where(sub8 == r + 1, det * ratio, diag))
            mixing = jnp.where(sub8 == r + 1, p01 * ratio, mixing)
            if r == 6:
                diags.append(diag)
                mixings.append(mixing)
            if j + 2 < BLOCK:
                share = 1.0 / det
                new0 = (p11 * row0 - p01 * row1) * share
                new1 = (p00 * row1 - p01 * row0) * share
                wide0[0] = jnp.where(sub8 > r + 1, wide0[0], 0.0)
                wide1[0] = jnp.where(sub8 > r + 1, wide1[0], 0.0)
                for i in range(at, len(tiles)):
                    tiles[i] = tiles[i] - (wide0[i - at] * new0 + wide1[i - at] * new1)
        small = jnp.concatenate(
            [
                (tile - mixing * pltpu.roll(tile, 1, 0)) * lax.rsqrt(diag)
                for tile, diag, mixing in zip(tiles, diags, mixings)
            ],
            0,
        )
        inverse = small[:, BLOCK : 2 * BLOCK]
        panel = nn(inverse, rows, highest)
        out[pl.ds(start, BLOCK), :] = panel[:, width:]
        lanes = iota((BLOCK, width), 1)
        below = jnp.where(lanes >= start + BLOCK, panel[:, :width], 0.0)
        ph, pm, pw = split3(below)
        qh, qm, qw = split3(panel)
        left_side = jnp.concatenate([ph, ph, pm, ph, pw, pm], 0)
        right_side = jnp.concatenate([qh, qm, qh, qw, qh, qm], 0)
        work[...] -= tn(left_side, right_side)
        return carry

    lax.fori_loop(0, width // BLOCK, block_step, 0)


def load_matrix(work, matrix, ridge):
    width = matrix.shape[0]
    eye = jnp.where(iota((width, width), 0) == iota((width, width), 1), 1.0, 0.0)
    if ridge is None:
        ridge = shrink_share * jnp.sum(matrix * eye) / width
    work[:, :width] = matrix + ridge * eye
    work[:, width:] = eye


def leaf_kernel(y_ref, w_ref, work, inv):
    y = y_ref[...]
    width = y.shape[1]
    load_matrix(work, tn(y, y, highest), None)
    inverse_factor(work, inv, width)
    w_ref[...] = nt(inv[...], y, highest).astype(bf16)


def leaf_weights_of(y):
    rows, width = y.shape
    return pl.pallas_call(
        leaf_kernel,
        out_shape=jax.ShapeDtypeStruct((width, rows), bf16),
        in_specs=[VMEM_SPEC],
        out_specs=VMEM_SPEC,
        scratch_shapes=[pltpu.VMEM((width, 2 * width), f32), pltpu.VMEM((width, width), f32)],
    )(y)


def merge_kernel(inner_ridge, g_ref, phi_ref, w_ref, k_ref, work, inv):
    width = phi_ref.shape[1]
    aa, ab, bb = (g_ref[i * width : (i + 1) * width, :] for i in range(3))
    top, low = phi_ref[:width, :], phi_ref[width:, :]
    y_top = nn(aa, top, highest) + nn(ab, low, highest)
    y_low = tn(ab, top, highest) + nn(bb, low, highest)
    load_matrix(work, tn(y_top, y_top, highest) + tn(y_low, y_low, highest), None)
    inverse_factor(work, inv, width)
    w_top = nt(inv[...], y_top, highest)
    w_low = nt(inv[...], y_low, highest)
    w_ref[:, :width] = w_top
    w_ref[:, width:] = w_low
    wg_top = nn(w_top, aa, highest) + nt(w_low, ab, highest)
    wg_low = nn(w_top, ab, highest) + nn(w_low, bb, highest)
    own_gram = nt(wg_top, w_top, highest) + nt(wg_low, w_low, highest)
    if inner_ridge is None:
        k_ref[...] = own_gram
        return
    load_matrix(work, own_gram, inner_ridge)
    inverse_factor(work, inv, width)
    k_ref[...] = tn(inv[...], inv[...], highest)


def merge_weights_of(gram, phi, inner_ridge):
    width = phi.shape[1]
    return pl.pallas_call(
        functools.partial(merge_kernel, inner_ridge),
        out_shape=(
            jax.ShapeDtypeStruct((width, 2 * width), f32),
            jax.ShapeDtypeStruct((width, width), f32),
        ),
        in_specs=[VMEM_SPEC] * 2,
        out_specs=(VMEM_SPEC,) * 2,
        scratch_shapes=[pltpu.VMEM((width, 2 * width), f32), pltpu.VMEM((width, width), f32)],
    )(gram, phi)


def small_sum_kernel(axis, n, x_ref, o_ref, land, send_sem, recv_sem):
    me = lax.axis_index(axis)
    barrier = pltpu.get_barrier_semaphore()
    for d in range(1, n):
        pl.semaphore_signal(barrier, inc=1, device_id={axis: lax.rem(me + d, n)}, device_id_type=MESH)
    pl.semaphore_wait(barrier, n - 1)
    for d in range(1, n):
        pltpu.make_async_remote_copy(
            x_ref, land.at[me], send_sem.at[d], recv_sem.at[me],
            device_id={axis: lax.rem(me + d, n)}, device_id_type=MESH,
        ).start()
    land[me] = x_ref[...]
    for d in range(1, n):
        source = lax.rem(me + n - d, n)
        pltpu.make_async_remote_copy(
            x_ref, land.at[source], send_sem.at[d], recv_sem.at[source],
            device_id={axis: lax.rem(me + d, n)}, device_id_type=MESH,
        ).wait()
    total = land[0]
    for i in range(1, n):
        total = total + land[i]
    o_ref[...] = total


def small_sum(x, axis, collective_id):
    n = lax.axis_size(axis)
    return pl.pallas_call(
        functools.partial(small_sum_kernel, axis, n),
        out_shape=jax.ShapeDtypeStruct(x.shape, f32),
        in_specs=[VMEM_SPEC],
        out_specs=VMEM_SPEC,
        scratch_shapes=[
            pltpu.VMEM((n, *x.shape), f32),
            pltpu.SemaphoreType.DMA((n,)),
            pltpu.SemaphoreType.DMA((n,)),
        ],
        compiler_params=pltpu.CompilerParams(collective_id=collective_id, has_side_effects=True),
    )(x)


def big_sum_kernel(n, share, x_ref, o_ref, land1, out1, land2, full, s1, r1, s2, r2, sa, ra, sb, rb, sc, rc, sd, rd):
    me = lax.axis_index("cols")
    position = lax.axis_index("rows")
    base = position // share * share
    own = lax.rem(position, share)
    side, line, far = lax.rem(me, 2), me // 2, n // 2
    other = 1 - side
    halves = max(share // 2, 1)
    chunk = x_ref.shape[0] // (n * share)

    def rows_of(line_at, side_at, sub):
        return pl.ds(pl.multiple_of((sub * n + line_at * 2 + side_at) * chunk, chunk), chunk)

    def along(t):
        return lax.rem(line + t, far)

    def back(t):
        return lax.rem(line + far - t, far)

    def sub_of(e, mine):
        return lax.rem(mine + share - 2 * e, share)

    pair = {"rows": position, "cols": line * 2 + other}
    sibling = {"rows": base + own + 1 - 2 * lax.rem(own, 2), "cols": me}
    sibling_own = own + 1 - 2 * lax.rem(own, 2)

    def peer(t, e):
        return {"rows": base + lax.rem(own + 2 * e, share), "cols": along(t) * 2 + side}

    spread = [(t, e) for e in range(halves) for t in range(far)]
    greeted = [pair] + [peer(t, e) for t, e in spread if t or e] + ([sibling] if share > 1 else [])
    barrier = pltpu.get_barrier_semaphore()
    for device in greeted:
        pl.semaphore_signal(barrier, inc=1, device_id=device, device_id_type=MESH)
    pl.semaphore_wait(barrier, len(greeted))

    def copy(src, dst, send, recv, device):
        return pltpu.make_async_remote_copy(src, dst, send, recv, device_id=device, device_id_type=MESH)

    first = []
    for t in range(far):
        rows = rows_of(along(t + 1), other, own)
        first.append(copy(x_ref.at[rows], land1.at[t], s1.at[t], r1.at[t], pair))
        first[-1].start()
    second = []
    for t in range(far):
        first[t].wait_recv()
        total = land1[t] + x_ref[rows_of(along(t + 1), side, own), :]
        if t + 1 < far:
            out1[t] = total
            second.append(copy(out1.at[t], land2.at[t], s2.at[t], r2.at[t], peer(t + 1, 0)))
            second[-1].start()
    for t in range(far - 1):
        second[t].wait_recv()
        total = total + land2[t]
    mine = rows_of(line, side, own)
    full[mine, :] = total

    outward, started = {}, []
    for t, e in spread:
        if t or e:
            outward[t, e] = copy(full.at[mine], full.at[mine], sa.at[t, e], ra.at[t, e], peer(t, e))
            outward[t, e].start()
    for t, e in spread:
        rows = rows_of(back(t), side, sub_of(e, own))
        if t or e:
            copy(full.at[mine], full.at[rows], sa.at[t, e], ra.at[t, e], peer(t, e)).wait_recv()
        started.append(copy(full.at[rows], full.at[rows], sb.at[t, e], rb.at[t, e], pair))
        started[-1].start()
        if share > 1:
            started.append(copy(full.at[rows], full.at[rows], sc.at[t, e], rc.at[t, e], sibling))
            started[-1].start()
    for t, e in spread:
        rows = rows_of(back(t), other, sub_of(e, own))
        copy(full.at[rows], full.at[rows], sb.at[t, e], rb.at[t, e], pair).wait_recv()
        if share > 1:
            started.append(copy(full.at[rows], full.at[rows], sd.at[t, e], rd.at[t, e], sibling))
            started[-1].start()
    if share > 1:
        for t, e in spread:
            rows = rows_of(back(t), side, sub_of(e, sibling_own))
            copy(full.at[rows], full.at[rows], sc.at[t, e], rc.at[t, e], sibling).wait_recv()
            rows = rows_of(back(t), other, sub_of(e, sibling_own))
            copy(full.at[rows], full.at[rows], sd.at[t, e], rd.at[t, e], sibling).wait_recv()
    for sent in first + second + list(outward.values()) + started:
        sent.wait_send()
    o_ref[...] = full[...]


def big_sum(x, share, collective_id):
    n = lax.axis_size("cols")
    while share > 1 and x.shape[0] % (n * share * 8):
        share //= 2
    chunk = x.shape[0] // (n * share)
    far, halves = n // 2, max(share // 2, 1)
    dma = pltpu.SemaphoreType.DMA
    return pl.pallas_call(
        functools.partial(big_sum_kernel, n, share),
        out_shape=jax.ShapeDtypeStruct(x.shape, f32),
        in_specs=[VMEM_SPEC],
        out_specs=VMEM_SPEC,
        scratch_shapes=[
            pltpu.VMEM((far, chunk, x.shape[1]), f32),
            pltpu.VMEM((far, chunk, x.shape[1]), f32),
            pltpu.VMEM((far, chunk, x.shape[1]), f32),
            pltpu.VMEM(x.shape, f32),
        ]
        + [dma((far,))] * 4
        + [dma((far, halves))] * 8,
        compiler_params=pltpu.CompilerParams(collective_id=collective_id, has_side_effects=True),
    )(x)


PIECES = 8


def swap_kernel(stride, x_ref, o_ref, land, ss, rs, fs, fr):
    position = lax.axis_index("rows")
    core = lax.rem(position, 2)
    partner = {"rows": position + stride - 2 * stride * lax.rem(position // stride, 2)}
    sibling = {"rows": position + 1 - 2 * core}
    piece = x_ref.shape[0] // (2 * PIECES)
    barrier = pltpu.get_barrier_semaphore()
    for device in (partner, sibling):
        pl.semaphore_signal(barrier, inc=1, device_id=device, device_id_type=MESH)
    pl.semaphore_wait(barrier, 2)

    def rows_of(half, i):
        return pl.ds(pl.multiple_of((half * PIECES + i) * piece, piece), piece)

    sent = []
    for i in range(PIECES):
        rows = rows_of(core, i)
        sent.append(
            pltpu.make_async_remote_copy(
                x_ref.at[rows], land.at[rows], ss.at[i], rs.at[i], device_id=partner, device_id_type=MESH
            )
        )
        sent[-1].start()
    passed = []
    for i in range(PIECES):
        rows = rows_of(core, i)
        sent[i].wait_recv()
        passed.append(
            pltpu.make_async_remote_copy(
                land.at[rows], land.at[rows], fs.at[i], fr.at[i], device_id=sibling, device_id_type=MESH
            )
        )
        passed[-1].start()
    for i in range(PIECES):
        rows = rows_of(1 - core, i)
        pltpu.make_async_remote_copy(
            land.at[rows], land.at[rows], fs.at[i], fr.at[i], device_id=sibling, device_id_type=MESH
        ).wait_recv()
    for copy in sent + passed:
        copy.wait_send()
    o_ref[...] = land[...]


def split_swap(x, stride, collective_id):
    dma = pltpu.SemaphoreType.DMA
    return pl.pallas_call(
        functools.partial(swap_kernel, stride),
        out_shape=jax.ShapeDtypeStruct(x.shape, f32),
        in_specs=[VMEM_SPEC],
        out_specs=VMEM_SPEC,
        scratch_shapes=[pltpu.VMEM(x.shape, f32)] + [dma((PIECES,))] * 4,
        compiler_params=pltpu.CompilerParams(collective_id=collective_id, has_side_effects=True),
    )(x)


def fold(value):
    total = value[:, :LANES]
    for i in range(1, value.shape[1] // LANES):
        total = total + value[:, i * LANES : (i + 1) * LANES]
    return total


def total_of(value):
    return jnp.sum(value, axis=1, keepdims=True)


def three_rows(value):
    wide = jnp.broadcast_to(value, (16, value.shape[1]))
    high = wide.astype(bf16).astype(f32)
    mid = (wide - high).astype(bf16).astype(f32)
    low = wide - high - mid
    sub = iota(wide.shape, 0)
    return jnp.where(sub == 0, high, jnp.where(sub == 1, mid, jnp.where(sub == 2, low, 0.0))).astype(bf16)


def many_rows(value):
    return jnp.broadcast_to(value, (16, value.shape[1])).astype(bf16)


def solve_kernel(
    n_rows, n_cols, samples,
    design, weight, scale, theta, misfit, sketch, kinv, out,
    s3, k3, a_send, a_land, b_send, b_land, c_send, c_land,
    a_ss, a_rs, b_ss, b_rs, c_ss, c_rs,
):
    width = sketch.shape[0]
    here = {"rows": lax.axis_index("rows"), "cols": lax.axis_index("cols")}
    sizes = {"rows": n_rows, "cols": n_cols}

    def peer(axis, d):
        return lax.rem(here[axis] + d, sizes[axis])

    barrier = pltpu.get_barrier_semaphore()
    for axis, n in sizes.items():
        for d in range(1, n):
            pl.semaphore_signal(barrier, inc=1, device_id={axis: peer(axis, d)}, device_id_type=MESH)
    pl.semaphore_wait(barrier, n_rows + n_cols - 2)

    def exchange(axis, value, parity, send, land, ss, rs):
        n, me = sizes[axis], here[axis]
        send[...] = value
        for d in range(1, n):
            pltpu.make_async_remote_copy(
                send, land.at[parity, me], ss.at[d], rs.at[parity, me],
                device_id={axis: peer(axis, d)}, device_id_type=MESH,
            ).start()
        land[parity, me] = value
        for d in range(1, n):
            source = peer(axis, n - d)
            pltpu.make_async_remote_copy(
                send, land.at[parity, source], ss.at[d], rs.at[parity, source],
                device_id={axis: peer(axis, d)}, device_id_type=MESH,
            ).wait()
        total = land[parity, 0]
        for i in range(1, n):
            total = total + land[parity, i]
        return total

    def precondition(vector, parity):
        left = three_rows(vector)
        parts = nt(left, s3[0]) + nt(left, s3[1]) + nt(left, s3[2])
        projected = jnp.sum(parts, axis=0, keepdims=True)
        both = jnp.concatenate([projected, fold(vector * vector)], 1)
        both = exchange("cols", both, parity, c_send, c_land, c_ss, c_rs)
        projected = both[:, :width]
        left = three_rows(projected)
        solved = jnp.sum(nn(left, k3[0]) + nn(left, k3[1]) + nn(left, k3[2]), axis=0, keepdims=True)
        left = three_rows(solved)
        removed = jnp.sum(nn(left, s3[0]) + nn(left, s3[1]) + nn(left, s3[2]), axis=0, keepdims=True)
        agreement = (total_of(both[:, width:]) - total_of(projected * solved)) / damping
        return (vector - removed) / damping, agreement

    def backward(inner, extra, parity):
        part = nn(many_rows(inner), design[...])[:1]
        both = jnp.concatenate([part, extra], 1)
        both = exchange("rows", both, parity, b_send, b_land, b_ss, b_rs)
        return scale[...] * both[:, : part.shape[1]] / samples, total_of(both[:, part.shape[1] :])

    for i, piece in enumerate(split3(sketch[...])):
        s3[i] = piece
    for i, piece in enumerate(split3(kinv[...])):
        k3[i] = piece

    scaled, _ = backward(misfit[...], jnp.zeros((1, LANES), f32), 1)
    residual = scaled + damping * theta[...]
    search, agreement = precondition(residual, 1)

    def advance(turn, search, residual, answer, agreement):
        parity = lax.rem(turn, 2)
        part = nt(many_rows(scale[...] * search), design[...])[:1]
        both = jnp.concatenate([part, fold(search * search)], 1)
        both = exchange("cols", both, parity, a_send, a_land, a_ss, a_rs)
        forward = both[:, : part.shape[1]]
        length = total_of(both[:, part.shape[1] :])
        inner = (weight[...] * forward).astype(bf16).astype(f32)
        product, bending = backward(inner, fold(forward * inner), parity)
        product = product + damping * search
        step_size = agreement / (bending / samples + damping * length)
        return residual - step_size * product, answer + step_size * search

    def body(turn, state):
        search, residual, answer, agreement = state
        residual, answer = advance(turn, search, residual, answer, agreement)
        smoothed, following = precondition(residual, lax.rem(turn, 2))
        return smoothed + following / agreement * search, residual, answer, following

    state = (search, residual, jnp.zeros_like(residual), agreement)
    search, residual, answer, agreement = lax.fori_loop(0, ITERS - 1, body, state)
    _, answer = advance(ITERS - 1, search, residual, answer, agreement)
    out[...] = answer


def solve(design, weight, scale, theta, misfit, sketch, kinv, collective_id):
    rows, cols = design.shape
    width = sketch.shape[0]
    n_rows, n_cols = lax.axis_size("rows"), lax.axis_size("cols")
    dma = pltpu.SemaphoreType.DMA
    return pl.pallas_call(
        functools.partial(solve_kernel, n_rows, n_cols, rows * n_rows),
        out_shape=jax.ShapeDtypeStruct((1, cols), f32),
        in_specs=[VMEM_SPEC] * 7,
        out_specs=VMEM_SPEC,
        scratch_shapes=[
            pltpu.VMEM((3, width, cols), bf16),
            pltpu.VMEM((3, width, width), bf16),
            pltpu.VMEM((1, rows + LANES), f32),
            pltpu.VMEM((2, n_cols, 1, rows + LANES), f32),
            pltpu.VMEM((1, cols + LANES), f32),
            pltpu.VMEM((2, n_rows, 1, cols + LANES), f32),
            pltpu.VMEM((1, width + LANES), f32),
            pltpu.VMEM((2, n_cols, 1, width + LANES), f32),
            dma((n_cols,)), dma((2, n_cols)),
            dma((n_rows,)), dma((2, n_rows)),
            dma((n_cols,)), dma((2, n_cols)),
        ],
        compiler_params=pltpu.CompilerParams(collective_id=collective_id, has_side_effects=True),
    )(design, weight, scale, theta, misfit, sketch, kinv)


def swapped(value, axis, stride):
    mask = 2**stride
    pairs = [(source, source ^ mask) for source in range(lax.axis_size(axis))]
    return lax.ppermute(value, axis, pairs)


def on_device(design, theta, feature_scale, labels, psi, phi):
    row_devices = lax.axis_size("rows")
    samples = design.shape[0] * row_devices
    width = psi.shape[1]
    scaled_theta = (theta * feature_scale).astype(bf16)
    part = jnp.dot(design, scaled_theta, preferred_element_type=f32)
    margins = small_sum(part.reshape(-1, LANES), "cols", 0).reshape(-1)
    chance = jax.nn.sigmoid(margins)
    weight = chance * (1.0 - chance)
    misfit = (chance - labels.astype(f32)).astype(bf16).astype(f32)
    rows_scaled = (
        design.astype(f32) * jnp.sqrt(weight)[:, None] * feature_scale[None, :]
    ).astype(bf16)
    mixed_cols = jnp.einsum("rf,rs->fs", rows_scaled, psi, preferred_element_type=f32).astype(bf16)
    range_rows = big_sum(jnp.dot(rows_scaled, mixed_cols, preferred_element_type=f32), 1, 1)
    sketch = jnp.dot(leaf_weights_of(range_rows), rows_scaled, preferred_element_type=f32)
    position = lax.axis_index("rows")
    levels = row_devices.bit_length() - 1
    features = sketch.shape[1]
    for level_bit in range(levels):
        if level_bit:
            sketch = jnp.concatenate([sketch, own_gram], 1)
            partner = split_swap(sketch, 1 << level_bit, 8 + level_bit)
        else:
            partner = swapped(sketch, "rows", level_bit)
        first_low = position // (1 << level_bit) % 2 == 0
        lower_half = jnp.where(first_low, sketch, partner)
        upper_half = jnp.where(first_low, partner, sketch)
        lower, upper = lower_half[:, :features], upper_half[:, :features]
        gram = jnp.dot(lower, upper.T, precision=highest)
        if level_bit:
            gram = big_sum(gram, 2 << level_bit, 2 + level_bit)
            gram = jnp.concatenate([lower_half[:, features:], gram, upper_half[:, features:]], 0)
        else:
            gram = jnp.concatenate(
                [
                    jnp.dot(lower, lower.T, precision=highest),
                    gram,
                    jnp.dot(upper, upper.T, precision=highest),
                ],
                0,
            )
            gram = big_sum(gram, 2, 2)
        last = level_bit + 1 == levels
        weights, own_gram = merge_weights_of(gram, phi, damping * samples if last else None)
        sketch = jnp.dot(weights, jnp.concatenate([lower, upper], 0), precision=highest)
    answer = solve(
        design, weight[None], feature_scale[None], theta[None], misfit[None], sketch, own_gram, 2 + levels
    )
    return answer[0], sketch


def solution(mesh):
    in_specs = (P("rows", "cols"), P("cols"), P("cols"), P("rows"), P(), P())
    out_specs = (P("cols"), P(None, "cols"))
    return jax.shard_map(
        on_device, mesh=mesh, in_specs=in_specs, out_specs=out_specs, check_vma=False
    )
```
